32 devices in a mesh: groups: 2 (over y), pair: 4 (over z), tp: 4 (over x, core).
Axes of the slice: x: 2, y: 2, z: 4, core: 2. Of those that a mesh axis runs over, the one named last changes fastest.
Arguments:
- prompt_keys: bfloat16 [8, 1536, 8, 128], P(('groups', 'pair'), None, 'tp'), parts along dimension 0, may hold values from -6 to 6
- prompt_values: bfloat16 [8, 1536, 8, 128], P(('groups', 'pair'), None, 'tp'), parts along dimension 0, may hold values from -6 to 6
- span_queries: bfloat16 [8, 512, 64, 128], P(('groups', 'pair'), None, 'tp'), parts along dimension 0, may hold values from -1024 to 1024
- span_keys: bfloat16 [8, 512, 8, 128], P(('groups', 'pair'), None, 'tp'), parts along dimension 0, may hold values from -6 to 6
- span_values: bfloat16 [8, 512, 8, 128], P(('groups', 'pair'), None, 'tp'), parts along dimension 0, may hold values from -6 to 6
- prefill_residual: bfloat16 [8, 512, 8192], P(('groups', 'pair'), None, 'tp'), parts along dimension 0, may hold values from -8 to 8
- decode_queries: bfloat16 [8, 2, 32, 64, 128], P(('groups', 'pair'), None, None, 'tp'), parts along dimension 0, may hold values from -1024 to 1024
- decode_keys: bfloat16 [8, 2, 32, 8, 128], P(('groups', 'pair'), None, None, 'tp'), parts along dimension 0, may hold values from -16 to 16
- decode_values: bfloat16 [8, 2, 32, 8, 128], P(('groups', 'pair'), None, None, 'tp'), parts along dimension 0, may hold values from -6 to 6
- decode_residual: bfloat16 [8, 2, 32, 8192], P(('groups', 'pair'), None, None, 'tp'), parts along dimension 0, may hold values from -8 to 8
- cursor: int32 [8, 32], P(('groups', 'pair')), parts along dimension 0, may hold values from 1024 to 2048
- norm_gain: bfloat16 [8192], P('tp'), may hold values from 0.25 to 1.75
Outputs:
- prefill_normed: bfloat16 [8, 512, 8192], P(('groups', 'pair'), None, 'tp'), parts along dimension 0
- handed_keys: bfloat16 [8, 2048, 8, 128], P(('groups', 'pair'), None, 'tp'), parts along dimension 0
- handed_values: bfloat16 [8, 2048, 8, 128], P(('groups', 'pair'), None, 'tp'), parts along dimension 0
- decode_normed: bfloat16 [8, 2, 32, 8192], P(('groups', 'pair'), None, None, 'tp'), parts along dimension 0
The draws below stay inside these ranges and needn't reach their ends.
There are 2 independent parts, one for each index of `groups`. The reference program is written for one: setup_inputs(seed, part) draws one part's arguments, and reference() takes and returns one part's arrays. A program takes and returns all parts, laid end to end along the dimension named above; an argument that names none is the same for every part. Nothing has to cross between parts.
All inputs are finite; a program needn't handle non-finite values.
Results may differ from the reference program's by a relative error of at most 0.0034.
Values may be sent and summed in bfloat16 or wider, within the bound.
A program may use at most 128 MiB of HBM per device.

```python
import jax
import jax.numpy as jnp
from jax import lax

D = 8192
H = 64
KVH = 8
HD = 128
S = 2048
SPAN = 512
ROWS = 32
STEPS = 2
NPROMPT = 4
CTX = 1536


def clipped_normal(key, array_shape):
    return jnp.clip(jax.random.normal(key, array_shape, jnp.float32), -6.0, 6.0)


def cache_keys(key):
    array_shape = (NPROMPT, CTX, KVH, HD)
    return clipped_normal(jax.random.fold_in(key, 101), array_shape)


def draw_prompt_keys(key, part):
    return cache_keys(key).astype(jnp.bfloat16)


def draw_span_queries(key, part):
    base_draw = clipped_normal(jax.random.fold_in(key, 201), (NPROMPT, SPAN, H, HD))
    return base_draw.astype(jnp.bfloat16)


def decode_base(key):
    return clipped_normal(jax.random.fold_in(key, 301), (NPROMPT, STEPS, ROWS, H, HD))


def draw_decode_queries(key, part):
    base_draw = decode_base(key)
    return base_draw.astype(jnp.bfloat16)


def draw_decode_keys(key, part):
    groups = H // KVH
    base_draw = decode_base(key).reshape(NPROMPT, STEPS, ROWS, KVH, groups, HD)
    summed = jnp.sum(base_draw, axis=4) * (1.2 / groups ** 0.5)
    jitter_term = clipped_normal(jax.random.fold_in(key, 303), summed.shape)
    return (summed + 0.3 * jitter_term).astype(jnp.bfloat16)


def spread_rows(key, array_shape):
    feature_count = array_shape[-1]
    position = jnp.arange(feature_count, dtype=jnp.float32) / (feature_count - 1)
    row_shape = array_shape[:-1] + (1,)
    entries = clipped_normal(jax.random.fold_in(key, 1), array_shape)
    feature_trend = 3.0 ** (0.5 * position)
    column_spread = 10.0 ** (0.5 * jax.random.uniform(jax.random.fold_in(key, 2), (feature_count,), jnp.float32))
    row_spread = 10.0 ** (0.5 * jax.random.uniform(jax.random.fold_in(key, 3), row_shape, jnp.float32))
    return 0.03 * entries * feature_trend * column_spread * row_spread


def draw_prefill_residual(key, part):
    return spread_rows(jax.random.fold_in(key, 401), (NPROMPT, SPAN, D)).astype(jnp.bfloat16)


def draw_decode_residual(key, part):
    return spread_rows(jax.random.fold_in(key, 501), (NPROMPT, STEPS, ROWS, D)).astype(jnp.bfloat16)


def place_ends(result, key, least, high):
    place = [jax.random.randint(jax.random.fold_in(key, axis), (), 0, length) for axis, length in enumerate(result.shape)]
    main_axis = result.shape.index(max(result.shape))
    neighbour = place[:main_axis] + [(place[main_axis] + 1) % result.shape[main_axis]] + place[main_axis + 1:]
    return result.at[tuple(place)].set(least).at[tuple(neighbour)].set(high)


def steps_of(stream_key, dims, split, smallest, top_value):
    loudness = 1.0
    for axis_at, shards_of in split:
        steps = jax.random.uniform(jax.random.fold_in(jax.random.fold_in(stream_key, 6), axis_at), (shards_of,), jnp.float32, smallest / len(split), top_value / len(split))
        loudness = loudness * jnp.repeat(jnp.exp(steps), dims[axis_at] // shards_of).reshape((-1,) + (1,) * (len(dims) - 1 - axis_at))
    return loudness


def gaussian(own_key, dims, spread, limit, cuts=(), held_as=jnp.bfloat16):
    drawn = jax.random.normal(own_key, dims, jnp.float32) * spread
    if len(cuts) > 0:
        drawn = steps_of(own_key, dims, cuts, -0.22, 0.18) * drawn
    return jnp.clip(drawn, min=-limit, max=limit).astype(held_as)


def setup_inputs(seed: int = 0, part: int = 0) -> dict:
    splits = jax.random.split(jax.random.key(seed), 13)
    part_splits = jax.random.split(jax.random.fold_in(splits[12], part), 13)
    return {
        "prompt_keys": draw_prompt_keys(jax.random.fold_in(jax.random.fold_in(splits[12], part), 71), part),
        "prompt_values": gaussian(part_splits[1], (NPROMPT, CTX, KVH, HD), 1.0, 6.0, ((0, 4), (2, 4))),
        "span_queries": draw_span_queries(jax.random.fold_in(jax.random.fold_in(splits[12], part), 71), part),
        "span_keys": gaussian(part_splits[3], (NPROMPT, SPAN, KVH, HD), 1.0, 6.0, ((0, 4), (2, 4))),
        "span_values": gaussian(part_splits[4], (NPROMPT, SPAN, KVH, HD), 1.0, 6.0, ((0, 4), (2, 4))),
        "prefill_residual": draw_prefill_residual(jax.random.fold_in(jax.random.fold_in(splits[12], part), 71), part),
        "decode_queries": draw_decode_queries(jax.random.fold_in(jax.random.fold_in(splits[12], part), 71), part),
        "decode_keys": draw_decode_keys(jax.random.fold_in(jax.random.fold_in(splits[12], part), 71), part),
        "decode_values": gaussian(part_splits[8], (NPROMPT, STEPS, ROWS, KVH, HD), 1.0, 6.0, ((0, 4), (3, 4))),
        "decode_residual": draw_decode_residual(jax.random.fold_in(jax.random.fold_in(splits[12], part), 71), part),
        "cursor": place_ends(jax.random.randint(part_splits[10], (NPROMPT, ROWS), S // 2, S + 1), jax.random.fold_in(part_splits[10], 1), S // 2, S).astype(jnp.int32),
        "norm_gain": jnp.clip(1.0 + 0.15 * jax.random.normal(splits[11], (D,), jnp.float32), 0.25, 1.75).astype(jnp.bfloat16),
    }


epsilon = 1e-05

def normalize(hidden, gain_wide):
    squares = lax.optimization_barrier(jnp.mean(hidden * hidden, axis=-1, keepdims=True))
    return (hidden * lax.rsqrt(squares + epsilon) * gain_wide).astype(jnp.bfloat16)

def prefill_attention(queries, keys_one, values_one):
    span_len = queries.shape[0]
    query_heads = queries.shape[1]
    head_size = queries.shape[2]
    key_heads = keys_one.shape[1]
    positions = keys_one.shape[0]
    groups = query_heads // key_heads
    score_scale = head_size ** (-0.5)
    row_index = jnp.arange(span_len, dtype=jnp.int32)[:, None] + (positions - span_len)
    col_index = jnp.arange(positions, dtype=jnp.int32)[None, :]
    visible = col_index <= row_index

    def one_head(head_index):
        query = lax.dynamic_index_in_dim(queries, head_index, 1, keepdims=False)
        key_head = lax.dynamic_index_in_dim(keys_one, head_index // groups, 1, keepdims=False)
        value_head = lax.dynamic_index_in_dim(values_one, head_index // groups, 1, keepdims=False)
        scores = jnp.dot(query, key_head.T, preferred_element_type=jnp.float32) * score_scale
        scores = jnp.where(visible, scores, -jnp.inf)
        row_max = lax.optimization_barrier(jnp.max(scores, axis=1, keepdims=True))
        scaled = jnp.exp(scores - row_max)
        denominator = lax.optimization_barrier(jnp.sum(scaled, axis=1, keepdims=True))
        weights = scaled.astype(jnp.bfloat16)
        return jnp.dot(weights, value_head, preferred_element_type=jnp.float32) / denominator
    per_head = lax.map(one_head, jnp.arange(query_heads, dtype=jnp.int32))
    return jnp.transpose(per_head, (1, 0, 2)).reshape(span_len, query_heads * head_size)

def decode_attention(queries, own_keys, own_values, reach_count, keys_one, values_one):
    steps_count, row_count, query_heads, head_size = queries.shape
    key_heads = keys_one.shape[1]
    positions = keys_one.shape[0]
    groups = query_heads // key_heads
    score_scale = head_size ** (-0.5)
    grouped = queries.astype(jnp.float32).reshape(steps_count, row_count, key_heads, groups, head_size)
    far_scores = jnp.einsum('trkgd,skd->trkgs', grouped, keys_one.astype(jnp.float32)) * score_scale
    reach = jnp.arange(positions, dtype=jnp.int32)[None, :] < reach_count[:, None]
    far_scores = jnp.where(reach[None, :, None, None, :], far_scores, -jnp.inf)
    own_scores = jnp.einsum('trkgd,urkd->trkgu', grouped, own_keys.astype(jnp.float32)) * score_scale
    earlier = jnp.arange(steps_count)[None, :] <= jnp.arange(steps_count)[:, None]
    own_scores = jnp.where(earlier[:, None, None, None, :], own_scores, -jnp.inf)
    row_max = jnp.maximum(lax.optimization_barrier(jnp.max(far_scores, axis=4)), lax.optimization_barrier(jnp.max(own_scores, axis=4)))[..., None]
    far_expon = jnp.exp(far_scores - row_max)
    own_expon = jnp.exp(own_scores - row_max)
    denominator = lax.optimization_barrier(jnp.sum(far_expon, axis=4)) + lax.optimization_barrier(jnp.sum(own_expon, axis=4))
    far_weights = far_expon.astype(jnp.bfloat16).astype(jnp.float32)
    own_weights = own_expon.astype(jnp.bfloat16).astype(jnp.float32)
    attended = jnp.einsum('trkgs,skd->trkgd', far_weights, values_one.astype(jnp.float32))
    attended = attended + jnp.einsum('trkgu,urkd->trkgd', own_weights, own_values.astype(jnp.float32))
    attended = attended / denominator[..., None]
    return attended.reshape(steps_count, row_count, query_heads * head_size)

def reference(prompt_keys, prompt_values, span_queries, span_keys, span_values, prefill_residual, decode_queries, decode_keys, decode_values, decode_residual, cursor, norm_gain):
    keys_all = jnp.concatenate([prompt_keys, span_keys], axis=1)
    values_all = jnp.concatenate([prompt_values, span_values], axis=1)
    gain_wide = norm_gain.astype(jnp.float32)

    def prefill_one(inputs):
        queries, keys_one, values_one, residual = inputs
        hidden = prefill_attention(queries, keys_one, values_one) + residual.astype(jnp.float32)
        return normalize(hidden, gain_wide)
    prefill_normed = lax.map(prefill_one, (span_queries, keys_all, values_all, prefill_residual))
    handed_keys = jnp.roll(keys_all, -(NPROMPT // 2), axis=0)
    handed_values = jnp.roll(values_all, -(NPROMPT // 2), axis=0)

    def decode_one(inputs):
        queries, own_keys, own_values, reach_count, keys_one, values_one, residual = inputs
        hidden = decode_attention(queries, own_keys, own_values, reach_count, keys_one, values_one) + residual.astype(jnp.float32)
        return normalize(hidden, gain_wide)
    decode_normed = lax.map(decode_one, (decode_queries, decode_keys, decode_values, cursor, handed_keys, handed_values, decode_residual))
    return (prefill_normed, handed_keys, handed_values, decode_normed)
```

```python
import functools

import jax
import jax.numpy as jnp
from jax import lax
from jax.experimental import pallas as pl
from jax.experimental.pallas import tpu as pltpu
from jax.sharding import PartitionSpec as P


epsilon = 1e-05
NT = (((1,), (1,)), ((), ()))
MESH = pl.DeviceIdType.MESH


def from_behind(value, axis, steps):
    count = lax.axis_size(axis)
    pairs = [(source, (source + steps) % count) for source in range(count)]
    return lax.ppermute(value, axis, pairs)


def prefill_kernel(block, past, scale, q_ref, k_ref, v_ref, res_ref, hid_ref, sq_ref):
    span, _ = q_ref.shape[1:]

    @pl.when(pl.program_id(0) == 0)
    def _():
        sq_ref[...] = jnp.zeros_like(sq_ref)

    for start in range(0, span, block):
        rows = slice(start, start + block)
        reach = past + start + block
        scores = lax.dot_general(
            q_ref[0, rows, :], k_ref[0, :reach, :], NT, preferred_element_type=jnp.float32
        )
        row = lax.broadcasted_iota(jnp.int32, (block, block), 0)
        col = lax.broadcasted_iota(jnp.int32, (block, block), 1)
        last = jnp.where(col <= row, scores[:, reach - block :], -jnp.inf)
        scores = jnp.concatenate([scores[:, : reach - block], last], axis=1)
        peak = jnp.max(scores, axis=1, keepdims=True)
        weights = jnp.exp((scores - peak) * scale)
        total = jnp.sum(weights, axis=1, keepdims=True)
        mixed = jnp.dot(
            weights.astype(jnp.bfloat16), v_ref[0, :reach, :], preferred_element_type=jnp.float32
        )
        hidden = mixed / total + res_ref[rows, :].astype(jnp.float32)
        hid_ref[rows, :] = hidden
        sq_ref[rows, :] += hidden * hidden


def prefill(queries, keys, values, residual):
    heads, span, head = queries.shape
    key_heads, positions, _ = keys.shape
    group = heads // key_heads
    block = min(256, span)
    return pl.pallas_call(
        functools.partial(prefill_kernel, block, positions - span, head ** (-0.5)),
        grid=(heads,),
        in_specs=[
            pl.BlockSpec((1, span, head), lambda h: (h, 0, 0)),
            pl.BlockSpec((1, positions, head), lambda h: (h // group, 0, 0)),
            pl.BlockSpec((1, positions, head), lambda h: (h // group, 0, 0)),
            pl.BlockSpec((span, head), lambda h: (0, h)),
        ],
        out_specs=[
            pl.BlockSpec((span, head), lambda h: (0, h)),
            pl.BlockSpec((span, head), lambda h: (0, 0)),
        ],
        out_shape=[
            jax.ShapeDtypeStruct((span, heads * head), jnp.float32),
            jax.ShapeDtypeStruct((span, head), jnp.float32),
        ],
        compiler_params=pltpu.CompilerParams(vmem_limit_bytes=40 * 2**20),
        cost_estimate=pl.CostEstimate(
            flops=8 * heads * span * positions * head,
            bytes_accessed=16 * 2**20,
            transcendentals=heads * span * positions,
        ),
        name="prefill",
    )(queries, keys, values, residual)


def weigh_kernel(
    scale, key_heads, steps, q_ref, pk_ref, sk_ref, dk_ref, dv_ref, cur_ref,
    w_ref, last_ref, inv_ref, own_ref, hk_ref,
):
    g = pl.program_id(0)
    first = jnp.logical_and(g == 0, pl.program_id(1) == 0)
    past = pk_ref.shape[0]

    @pl.when(first)
    def _():
        hk_ref[:past, :] = pk_ref[...]
        hk_ref[past:, :] = sk_ref[...]

    q = q_ref[0]
    rows = q.shape[0]
    scores = jnp.concatenate(
        [
            lax.dot_general(q, pk_ref[...], NT, preferred_element_type=jnp.float32),
            lax.dot_general(q, sk_ref[...], NT, preferred_element_type=jnp.float32),
        ],
        axis=1,
    )
    col = lax.broadcasted_iota(jnp.int32, scores.shape, 1)
    seen = jnp.logical_and(col % key_heads == g, col < cur_ref[...] * key_heads)
    scores = jnp.where(seen, scores, -jnp.inf)
    peak = jnp.max(scores, axis=1, keepdims=True)
    count = dk_ref.shape[2]
    copies = rows // count
    step = lax.broadcasted_iota(jnp.int32, (rows, 1), 0) // count % steps
    wide = q.astype(jnp.float32)
    own_scores = []
    for u in range(steps):
        key = jnp.concatenate([dk_ref[0, u].astype(jnp.float32)] * copies, axis=0)
        own = jnp.sum(wide * key, axis=1, keepdims=True)
        own = jnp.where(step >= u, own, -jnp.inf)
        own_scores.append(own)
        peak = jnp.maximum(peak, own)
    weights = jnp.exp((scores - peak) * scale)
    total = jnp.sum(weights, axis=1, keepdims=True)
    rounded = weights.astype(jnp.bfloat16)
    w_ref[0] = rounded[:, : w_ref.shape[2]]
    last_ref[0] = rounded[:, w_ref.shape[2] :]
    mixed = jnp.zeros(wide.shape, jnp.float32)
    for u in range(steps):
        value = jnp.concatenate([dv_ref[0, u].astype(jnp.float32)] * copies, axis=0)
        weight = jnp.exp((own_scores[u] - peak) * scale)
        total = total + weight
        mixed = mixed + weight.astype(jnp.bfloat16).astype(jnp.float32) * value
    inv_ref[0] = jnp.broadcast_to(1.0 / total, wide.shape)
    own_ref[0] = mixed


def weigh(queries, prompt_keys, span_keys, own_keys, own_values, reach, ending):
    key_heads, rows, head = queries.shape
    _, steps, count, _ = own_keys.shape
    past, span = prompt_keys.shape[0], span_keys.shape[0]
    block = reach.shape[0]
    return pl.pallas_call(
        functools.partial(weigh_kernel, head ** (-0.5), key_heads, steps),
        grid=(key_heads, rows // block),
        in_specs=[
            pl.BlockSpec((1, block, head), lambda g, i: (g, i, 0)),
            pl.BlockSpec((past, head), lambda g, i: (0, 0)),
            pl.BlockSpec((span, head), lambda g, i: (0, 0)),
            pl.BlockSpec((1, steps, count, head), lambda g, i: (g, 0, 0, 0)),
            pl.BlockSpec((1, steps, count, head), lambda g, i: (g, 0, 0, 0)),
            pl.BlockSpec((block, 1), lambda g, i: (0, 0)),
        ],
        out_specs=[
            pl.BlockSpec((1, block, past + span - ending), lambda g, i: (g, i, 0)),
            pl.BlockSpec((1, block, ending), lambda g, i: (g, i, 0)),
            pl.BlockSpec((1, block, head), lambda g, i: (g, i, 0)),
            pl.BlockSpec((1, block, head), lambda g, i: (g, i, 0)),
            pl.BlockSpec((past + span, head), lambda g, i: (0, 0)),
        ],
        out_shape=[
            jax.ShapeDtypeStruct((key_heads, rows, past + span - ending), jnp.bfloat16),
            jax.ShapeDtypeStruct((key_heads, rows, ending), jnp.bfloat16),
            jax.ShapeDtypeStruct((key_heads, rows, head), jnp.float32),
            jax.ShapeDtypeStruct((key_heads, rows, head), jnp.float32),
            jax.ShapeDtypeStruct((past + span, head), jnp.bfloat16),
        ],
        compiler_params=pltpu.CompilerParams(vmem_limit_bytes=40 * 2**20),
        cost_estimate=pl.CostEstimate(
            flops=4 * key_heads * rows * (past + span) * head,
            bytes_accessed=16 * 2**20,
            transcendentals=key_heads * rows * (past + span),
        ),
        name="weigh",
    )(queries, prompt_keys, span_keys, own_keys, own_values, reach)


def mix_kernel(w_ref, v_ref, own_ref, acc_ref, hv_ref):
    @pl.when(pl.program_id(0) == 0)
    def _():
        hv_ref[...] = v_ref[...]

    acc_ref[0] = own_ref[0] + jnp.dot(w_ref[0], v_ref[...], preferred_element_type=jnp.float32)


def mix(weights, prompt_values, own, both):
    key_heads, rows, _ = weights.shape
    past, head = prompt_values.shape
    return pl.pallas_call(
        mix_kernel,
        grid=(key_heads,),
        in_specs=[
            pl.BlockSpec((1, rows, past), lambda g: (g, 0, 0)),
            pl.BlockSpec((past, head), lambda g: (0, 0)),
            pl.BlockSpec((1, rows, head), lambda g: (g, 0, 0)),
        ],
        out_specs=[
            pl.BlockSpec((1, rows, head), lambda g: (g, 0, 0)),
            pl.BlockSpec((past, head), lambda g: (0, 0)),
        ],
        out_shape=[
            jax.ShapeDtypeStruct((key_heads, rows, head), jnp.float32),
            jax.ShapeDtypeStruct((both, head), jnp.bfloat16),
        ],
        compiler_params=pltpu.CompilerParams(vmem_limit_bytes=40 * 2**20),
        cost_estimate=pl.CostEstimate(
            flops=4 * key_heads * rows * past * head, bytes_accessed=8 * 2**20, transcendentals=0
        ),
        name="mix",
    )(weights, prompt_values, own)


def gather_kernel(w_ref, v_ref, acc_ref, inv_ref, res_ref, hv_in, part_ref, hv_ref):
    del hv_in

    @pl.when(pl.program_id(0) == 0)
    def _():
        hv_ref[...] = v_ref[...]

    mixed = acc_ref[0] + jnp.dot(w_ref[0], v_ref[...], preferred_element_type=jnp.float32)
    mixed = mixed * inv_ref[0]
    count = res_ref.shape[0]
    head = mixed.shape[1]
    for h in range(mixed.shape[0] // count):
        columns = slice(h * head, (h + 1) * head)
        part_ref[:, columns] = mixed[h * count : (h + 1) * count] + res_ref[:, columns].astype(jnp.float32)


def gather(weights, span_values, acc, inverse, residual, handed):
    key_heads, rows, _ = weights.shape
    span, head = span_values.shape
    both = handed.shape[0]
    count, width = residual.shape
    at = both // span - 2
    return pl.pallas_call(
        gather_kernel,
        grid=(key_heads,),
        in_specs=[
            pl.BlockSpec((1, rows, span), lambda g: (g, 0, at)),
            pl.BlockSpec((span, head), lambda g: (0, 0)),
            pl.BlockSpec((1, rows, head), lambda g: (g, 0, 0)),
            pl.BlockSpec((1, rows, head), lambda g: (g, 0, 0)),
            pl.BlockSpec((count, width // key_heads), lambda g: (0, g)),
            pl.BlockSpec(memory_space=pl.ANY),
        ],
        out_specs=[
            pl.BlockSpec((count, width // key_heads), lambda g: (0, g)),
            pl.BlockSpec((span, head), lambda g: (at, 0)),
        ],
        out_shape=[
            jax.ShapeDtypeStruct((count, width), jnp.float32),
            jax.ShapeDtypeStruct((both, head), jnp.bfloat16),
        ],
        input_output_aliases={5: 1},
        compiler_params=pltpu.CompilerParams(vmem_limit_bytes=40 * 2**20),
        cost_estimate=pl.CostEstimate(
            flops=4 * key_heads * rows * span * head, bytes_accessed=6 * 2**20, transcendentals=0
        ),
        name="gather",
    )(weights, span_values, acc, inverse, residual, handed)


def close_kernel(
    w_ref, v_ref, part_ref, inv_ref, hid_ref, sum_ref, mine, others, send_sem, recv_sem
):
    devices, me = lax.axis_size("tp"), lax.axis_index("tp")
    ahead = [{"tp": lax.rem(me + k, devices)} for k in range(1, devices)]
    barrier = pltpu.get_barrier_semaphore()
    for peer in ahead:
        pl.semaphore_signal(barrier, inc=1, device_id=peer, device_id_type=MESH)

    key_heads, rows, _ = w_ref.shape
    count = part_ref.shape[0]
    head = v_ref.shape[1]
    squares = jnp.zeros((count, head), jnp.float32)
    for g in range(key_heads):
        mixed = jnp.dot(w_ref[g], v_ref[...], preferred_element_type=jnp.float32) * inv_ref[g]
        for h in range(rows // count):
            at = (g * (rows // count) + h) * head
            hidden = part_ref[:, at : at + head] + mixed[h * count : (h + 1) * count]
            hid_ref[:, at : at + head] = hidden
            squares = squares + hidden * hidden
    sums = jnp.sum(squares, axis=1, keepdims=True)
    lane = lax.broadcasted_iota(jnp.int32, mine.shape, 1)
    tile = jnp.zeros(mine.shape, jnp.float32)
    for k in range(count // mine.shape[0]):
        tile = jnp.where(lane == k, sums[k * mine.shape[0] : (k + 1) * mine.shape[0]], tile)
    mine[...] = tile
    pl.semaphore_wait(barrier, devices - 1)
    copies = [
        pltpu.make_async_remote_copy(
            src_ref=mine,
            dst_ref=others.at[k],
            send_sem=send_sem.at[k],
            recv_sem=recv_sem.at[k],
            device_id=peer,
            device_id_type=MESH,
        )
        for k, peer in enumerate(ahead)
    ]
    for copy in copies:
        copy.start()
    for k, copy in enumerate(copies):
        copy.wait_recv()
        tile = tile + others[k]
    sum_ref[...] = tile
    for copy in copies:
        copy.wait_send()


def close(weights, values, part, inverse):
    count, width = part.shape
    key_heads, rows, span = weights.shape
    head = values.shape[1]
    peers = lax.axis_size("tp") - 1
    vmem = pl.BlockSpec(memory_space=pltpu.VMEM)
    return pl.pallas_call(
        close_kernel,
        in_specs=[vmem] * 4,
        out_specs=[vmem] * 2,
        out_shape=[
            jax.ShapeDtypeStruct((count, width), jnp.float32),
            jax.ShapeDtypeStruct((8, head), jnp.float32),
        ],
        scratch_shapes=[
            pltpu.VMEM((8, head), jnp.float32),
            pltpu.VMEM((peers, 8, head), jnp.float32),
            pltpu.SemaphoreType.DMA((peers,)),
            pltpu.SemaphoreType.DMA((peers,)),
        ],
        compiler_params=pltpu.CompilerParams(
            collective_id=0, has_side_effects=True, vmem_limit_bytes=40 * 2**20
        ),
        cost_estimate=pl.CostEstimate(
            flops=4 * key_heads * rows * span * head, bytes_accessed=4 * 2**20, transcendentals=0
        ),
        name="close",
    )(weights, values, part, inverse)


def write_kernel(
    width, hid_ref, sum_ref, gain_ref, v_ref, hv_in, out_ref, hv_ref, buffer, sems
):
    del hv_in
    span = v_ref.shape[0]
    both = hv_ref.shape[0]
    move = pltpu.make_async_copy(v_ref, hv_ref.at[pl.ds(both - span, span)], sems.at[0])
    move.start()
    scale = lax.rsqrt(sum_ref[...] / width + epsilon)
    tall = scale.shape[0]
    moves = [move]
    step = 2 * tall
    for n, start in enumerate(range(0, hid_ref.shape[0], step)):
        rows = slice(start, start + step)
        first = start // tall
        each = jnp.concatenate([scale[:, first + k : first + k + 1] for k in range(2)], axis=0)
        buffer[rows, :] = (hid_ref[rows, :] * each * gain_ref[...]).astype(jnp.bfloat16)
        out = pltpu.make_async_copy(buffer.at[pl.ds(start, step)], out_ref.at[pl.ds(start, step)], sems.at[n + 1])
        out.start()
        moves.append(out)
    for move in moves:
        move.wait()


def write(hidden, sums, gain, values, handed):
    count, columns = hidden.shape
    vmem = pl.BlockSpec(memory_space=pltpu.VMEM)
    anywhere = pl.BlockSpec(memory_space=pl.ANY)
    return pl.pallas_call(
        functools.partial(write_kernel, columns * lax.axis_size("tp")),
        in_specs=[vmem] * 4 + [anywhere],
        out_specs=[anywhere] * 2,
        out_shape=[
            jax.ShapeDtypeStruct((count, columns), jnp.bfloat16),
            jax.ShapeDtypeStruct(handed.shape, jnp.bfloat16),
        ],
        scratch_shapes=[
            pltpu.VMEM((count, columns), jnp.bfloat16),
            pltpu.SemaphoreType.DMA((1 + count // 16,)),
        ],
        input_output_aliases={4: 1},
        compiler_params=pltpu.CompilerParams(vmem_limit_bytes=40 * 2**20),
        cost_estimate=pl.CostEstimate(
            flops=8 * count * columns, bytes_accessed=2 * 2**20, transcendentals=0
        ),
        name="write",
    )(hidden, sums, gain, values, handed)


def normed(hidden, partial, gain):
    width = hidden.shape[1] * lax.axis_size("tp")
    squares = lax.psum(jnp.sum(partial, axis=1), "tp")
    scaled = hidden * lax.rsqrt(squares[:, None] / width + epsilon) * gain.astype(jnp.float32)
    return scaled.astype(jnp.bfloat16)


def local(
    prompt_keys,
    prompt_values,
    span_queries,
    span_keys,
    span_values,
    prefill_residual,
    decode_queries,
    decode_keys,
    decode_values,
    decode_residual,
    cursor,
    norm_gain,
):
    halfway = lax.axis_size("pair") // 2
    span, heads, head = span_queries.shape[1:]
    past, key_heads = prompt_keys.shape[1:3]
    steps, count = decode_keys.shape[1:3]
    group = heads // key_heads
    flat = lambda a: a.reshape(-1, head)
    far = []
    early = span // 2
    pieces = (prompt_keys, span_keys, prompt_values, span_values[:, :early], span_values[:, early:])
    for piece in pieces:
        far.append(from_behind(flat(piece), "pair", halfway))
    far_pk, far_sk, far_pv, far_sv, far_tv = far

    keys = jnp.concatenate([prompt_keys[0], span_keys[0]], axis=0).transpose(1, 0, 2)
    values = jnp.concatenate([prompt_values[0], span_values[0]], axis=0).transpose(1, 0, 2)
    queries = span_queries[0].transpose(1, 0, 2)
    prefill_hidden, prefill_partial = prefill(queries, keys, values, prefill_residual[0])
    prefill_out = normed(prefill_hidden, prefill_partial, norm_gain)

    dq = decode_queries[0].reshape(steps * count, heads, head).transpose(1, 0, 2)
    dq = dq.reshape(key_heads, group * steps * count, head)
    dk = decode_keys[0].transpose(2, 0, 1, 3)
    dv = decode_values[0].transpose(2, 0, 1, 3)
    block = steps * count * (2 if group % 2 == 0 else 1)
    reach = jnp.tile(cursor[0], block // count)[:, None]
    prefill_out, dq, dk, dv, reach = lax.optimization_barrier((prefill_out, dq, dk, dv, reach))
    weights, ending, inverse, own, handed_keys = weigh(
        dq, far_pk, far_sk, dk, dv, reach, far_tv.shape[0]
    )
    acc, handed = mix(weights, far_pv, own, (past + span) * key_heads)
    residual = decode_residual[0].reshape(steps * count, heads * head)
    part, handed = gather(weights, far_sv, acc, inverse, residual, handed)
    decode_hidden, sums = close(ending, far_tv, part, inverse)
    gain = norm_gain.astype(jnp.float32)[None, :]
    decode_out, handed_values = write(decode_hidden, sums, gain, far_tv, handed)
    shape = (1, past + span, key_heads, head)
    return (
        prefill_out[None],
        handed_keys.reshape(shape),
        handed_values.reshape(shape),
        decode_out.reshape(decode_residual.shape),
    )


def solution(mesh):
    row = ("groups", "pair")
    placed = (
        P(row, None, "tp", None),
        P(row, None, "tp", None),
        P(row, None, "tp", None),
        P(row, None, "tp", None),
        P(row, None, "tp", None),
        P(row, None, "tp"),
        P(row, None, None, "tp", None),
        P(row, None, None, "tp", None),
        P(row, None, None, "tp", None),
        P(row, None, None, "tp"),
        P(row, None),
        P("tp"),
    )
    return jax.shard_map(
        local,
        mesh=mesh,
        in_specs=placed,
        out_specs=(
            P(row, None, "tp"),
            P(row, None, "tp", None),
            P(row, None, "tp", None),
            P(row, None, None, "tp"),
        ),
        check_vma=False,
    )
```

```python
import functools

import jax
import jax.numpy as jnp
from jax import lax
from jax.experimental import pallas as pl
from jax.experimental.pallas import tpu as pltpu
from jax.sharding import PartitionSpec as P


epsilon = 1e-05
NT = (((1,), (1,)), ((), ()))
MESH = pl.DeviceIdType.MESH


def from_behind(value, axis, steps):
    count = lax.axis_size(axis)
    pairs = [(source, (source + steps) % count) for source in range(count)]
    return lax.ppermute(value, axis, pairs)


def prefill_kernel(block, past, scale, q_ref, k_ref, v_ref, res_ref, hid_ref, sq_ref):
    span, _ = q_ref.shape[1:]

    @pl.when(pl.program_id(0) == 0)
    def _():
        sq_ref[...] = jnp.zeros_like(sq_ref)

    for start in range(0, span, block):
        rows = slice(start, start + block)
        reach = past + start + block
        scores = lax.dot_general(
            q_ref[0, rows, :], k_ref[0, :reach, :], NT, preferred_element_type=jnp.float32
        )
        row = lax.broadcasted_iota(jnp.int32, (block, block), 0)
        col = lax.broadcasted_iota(jnp.int32, (block, block), 1)
        last = jnp.where(col <= row, scores[:, reach - block :], -jnp.inf)
        scores = jnp.concatenate([scores[:, : reach - block], last], axis=1)
        peak = jnp.max(scores, axis=1, keepdims=True)
        weights = jnp.exp((scores - peak) * scale)
        total = jnp.sum(weights, axis=1, keepdims=True)
        mixed = jnp.dot(
            weights.astype(jnp.bfloat16), v_ref[0, :reach, :], preferred_element_type=jnp.float32
        )
        hidden = mixed / total + res_ref[rows, :].astype(jnp.float32)
        hid_ref[rows, :] = hidden
        sq_ref[rows, :] += hidden * hidden


def prefill(queries, keys, values, residual):
    heads, span, head = queries.shape
    key_heads, positions, _ = keys.shape
    group = heads // key_heads
    block = min(256, span)
    return pl.pallas_call(
        functools.partial(prefill_kernel, block, positions - span, head ** (-0.5)),
        grid=(heads,),
        in_specs=[
            pl.BlockSpec((1, span, head), lambda h: (h, 0, 0)),
            pl.BlockSpec((1, positions, head), lambda h: (h // group, 0, 0)),
            pl.BlockSpec((1, positions, head), lambda h: (h // group, 0, 0)),
            pl.BlockSpec((span, head), lambda h: (0, h)),
        ],
        out_specs=[
            pl.BlockSpec((span, head), lambda h: (0, h)),
            pl.BlockSpec((span, head), lambda h: (0, 0)),
        ],
        out_shape=[
            jax.ShapeDtypeStruct((span, heads * head), jnp.float32),
            jax.ShapeDtypeStruct((span, head), jnp.float32),
        ],
        compiler_params=pltpu.CompilerParams(vmem_limit_bytes=40 * 2**20),
        cost_estimate=pl.CostEstimate(
            flops=8 * heads * span * positions * head,
            bytes_accessed=16 * 2**20,
            transcendentals=heads * span * positions,
        ),
        name="prefill",
    )(queries, keys, values, residual)


def weigh_kernel(
    scale, key_heads, steps, q_ref, pk_ref, sk_ref, dk_ref, dv_ref, cur_ref,
    w_ref, last_ref, inv_ref, own_ref, hk_ref,
):
    g = pl.program_id(0)
    first = jnp.logical_and(g == 0, pl.program_id(1) == 0)
    past = pk_ref.shape[0]

    @pl.when(first)
    def _():
        hk_ref[:past, :] = pk_ref[...]
        hk_ref[past:, :] = sk_ref[...]

    q = q_ref[0]
    rows = q.shape[0]
    scores = jnp.concatenate(
        [
            lax.dot_general(q, pk_ref[...], NT, preferred_element_type=jnp.float32),
            lax.dot_general(q, sk_ref[...], NT, preferred_element_type=jnp.float32),
        ],
        axis=1,
    )
    col = lax.broadcasted_iota(jnp.int32, scores.shape, 1)
    seen = jnp.logical_and(col % key_heads == g, col < cur_ref[...] * key_heads)
    scores = jnp.where(seen, scores, -jnp.inf)
    peak = jnp.max(scores, axis=1, keepdims=True)
    count = dk_ref.shape[2]
    copies = rows // count
    step = lax.broadcasted_iota(jnp.int32, (rows, 1), 0) // count % steps
    wide = q.astype(jnp.float32)
    own_scores = []
    for u in range(steps):
        key = jnp.concatenate([dk_ref[0, u].astype(jnp.float32)] * copies, axis=0)
        own = jnp.sum(wide * key, axis=1, keepdims=True)
        own = jnp.where(step >= u, own, -jnp.inf)
        own_scores.append(own)
        peak = jnp.maximum(peak, own)
    weights = jnp.exp((scores - peak) * scale)
    total = jnp.sum(weights, axis=1, keepdims=True)
    rounded = weights.astype(jnp.bfloat16)
    w_ref[0] = rounded[:, : w_ref.shape[2]]
    last_ref[0] = rounded[:, w_ref.shape[2] :]
    mixed = jnp.zeros(wide.shape, jnp.float32)
    for u in range(steps):
        value = jnp.concatenate([dv_ref[0, u].astype(jnp.float32)] * copies, axis=0)
        weight = jnp.exp((own_scores[u] - peak) * scale)
        total = total + weight
        mixed = mixed + weight.astype(jnp.bfloat16).astype(jnp.float32) * value
    inv_ref[0] = jnp.broadcast_to(1.0 / total, wide.shape)
    own_ref[0] = mixed


def weigh(queries, prompt_keys, span_keys, own_keys, own_values, reach, ending):
    key_heads, rows, head = queries.shape
    _, steps, count, _ = own_keys.shape
    past, span = prompt_keys.shape[0], span_keys.shape[0]
    block = reach.shape[0]
    return pl.pallas_call(
        functools.partial(weigh_kernel, head ** (-0.5), key_heads, steps),
        grid=(key_heads, rows // block),
        in_specs=[
            pl.BlockSpec((1, block, head), lambda g, i: (g, i, 0)),
            pl.BlockSpec((past, head), lambda g, i: (0, 0)),
            pl.BlockSpec((span, head), lambda g, i: (0, 0)),
            pl.BlockSpec((1, steps, count, head), lambda g, i: (g, 0, 0, 0)),
            pl.BlockSpec((1, steps, count, head), lambda g, i: (g, 0, 0, 0)),
            pl.BlockSpec((block, 1), lambda g, i: (0, 0)),
        ],
        out_specs=[
            pl.BlockSpec((1, block, past + span - ending), lambda g, i: (g, i, 0)),
            pl.BlockSpec((1, block, ending), lambda g, i: (g, i, 0)),
            pl.BlockSpec((1, block, head), lambda g, i: (g, i, 0)),
            pl.BlockSpec((1, block, head), lambda g, i: (g, i, 0)),
            pl.BlockSpec((past + span, head), lambda g, i: (0, 0)),
        ],
        out_shape=[
            jax.ShapeDtypeStruct((key_heads, rows, past + span - ending), jnp.bfloat16),
            jax.ShapeDtypeStruct((key_heads, rows, ending), jnp.bfloat16),
            jax.ShapeDtypeStruct((key_heads, rows, head), jnp.float32),
            jax.ShapeDtypeStruct((key_heads, rows, head), jnp.float32),
            jax.ShapeDtypeStruct((past + span, head), jnp.bfloat16),
        ],
        compiler_params=pltpu.CompilerParams(vmem_limit_bytes=40 * 2**20),
        cost_estimate=pl.CostEstimate(
            flops=4 * key_heads * rows * (past + span) * head,
            bytes_accessed=16 * 2**20,
            transcendentals=key_heads * rows * (past + span),
        ),
        name="weigh",
    )(queries, prompt_keys, span_keys, own_keys, own_values, reach)


def mix_kernel(w_ref, v_ref, own_ref, acc_ref, hv_ref):
    @pl.when(pl.program_id(0) == 0)
    def _():
        hv_ref[...] = v_ref[...]

    acc_ref[0] = own_ref[0] + jnp.dot(w_ref[0], v_ref[...], preferred_element_type=jnp.float32)


def mix(weights, prompt_values, own, both):
    key_heads, rows, _ = weights.shape
    past, head = prompt_values.shape
    return pl.pallas_call(
        mix_kernel,
        grid=(key_heads,),
        in_specs=[
            pl.BlockSpec((1, rows, past), lambda g: (g, 0, 0)),
            pl.BlockSpec((past, head), lambda g: (0, 0)),
            pl.BlockSpec((1, rows, head), lambda g: (g, 0, 0)),
        ],
        out_specs=[
            pl.BlockSpec((1, rows, head), lambda g: (g, 0, 0)),
            pl.BlockSpec((past, head), lambda g: (0, 0)),
        ],
        out_shape=[
            jax.ShapeDtypeStruct((key_heads, rows, head), jnp.float32),
            jax.ShapeDtypeStruct((both, head), jnp.bfloat16),
        ],
        compiler_params=pltpu.CompilerParams(vmem_limit_bytes=40 * 2**20),
        cost_estimate=pl.CostEstimate(
            flops=4 * key_heads * rows * past * head, bytes_accessed=8 * 2**20, transcendentals=0
        ),
        name="mix",
    )(weights, prompt_values, own)


def mix_more_kernel(w_ref, v_ref, own_ref, hv_in, acc_ref, hv_ref):
    del hv_in
    mix_kernel(w_ref, v_ref, own_ref, acc_ref, hv_ref)


def mix_more(weights, values, acc, handed, start):
    key_heads, rows, _ = weights.shape
    span, head = values.shape
    at = start // span
    return pl.pallas_call(
        mix_more_kernel,
        grid=(key_heads,),
        in_specs=[
            pl.BlockSpec((1, rows, span), lambda g: (g, 0, at)),
            pl.BlockSpec((span, head), lambda g: (0, 0)),
            pl.BlockSpec((1, rows, head), lambda g: (g, 0, 0)),
            pl.BlockSpec(memory_space=pl.ANY),
        ],
        out_specs=[
            pl.BlockSpec((1, rows, head), lambda g: (g, 0, 0)),
            pl.BlockSpec((span, head), lambda g: (at, 0)),
        ],
        out_shape=[
            jax.ShapeDtypeStruct((key_heads, rows, head), jnp.float32),
            jax.ShapeDtypeStruct(handed.shape, jnp.bfloat16),
        ],
        input_output_aliases={3: 1},
        compiler_params=pltpu.CompilerParams(vmem_limit_bytes=40 * 2**20),
        cost_estimate=pl.CostEstimate(
            flops=4 * key_heads * rows * span * head, bytes_accessed=6 * 2**20, transcendentals=0
        ),
        name="mix_more",
    )(weights, values, acc, handed)


def gather_kernel(w_ref, v_ref, acc_ref, inv_ref, res_ref, part_ref):
    mixed = acc_ref[0] + jnp.dot(w_ref[0], v_ref[...], preferred_element_type=jnp.float32)
    mixed = mixed * inv_ref[0]
    count = res_ref.shape[0]
    head = mixed.shape[1]
    for h in range(mixed.shape[0] // count):
        columns = slice(h * head, (h + 1) * head)
        part_ref[:, columns] = mixed[h * count : (h + 1) * count] + res_ref[:, columns].astype(jnp.float32)


def gather(weights, span_values, acc, inverse, residual):
    key_heads, rows, columns = weights.shape
    span, head = span_values.shape
    count, width = residual.shape
    at = columns // span - 1
    return pl.pallas_call(
        gather_kernel,
        grid=(key_heads,),
        in_specs=[
            pl.BlockSpec((1, rows, span), lambda g: (g, 0, at)),
            pl.BlockSpec((span, head), lambda g: (0, 0)),
            pl.BlockSpec((1, rows, head), lambda g: (g, 0, 0)),
            pl.BlockSpec((1, rows, head), lambda g: (g, 0, 0)),
            pl.BlockSpec((count, width // key_heads), lambda g: (0, g)),
        ],
        out_specs=pl.BlockSpec((count, width // key_heads), lambda g: (0, g)),
        out_shape=jax.ShapeDtypeStruct((count, width), jnp.float32),
        compiler_params=pltpu.CompilerParams(vmem_limit_bytes=40 * 2**20),
        cost_estimate=pl.CostEstimate(
            flops=4 * key_heads * rows * span * head, bytes_accessed=6 * 2**20, transcendentals=0
        ),
        name="gather",
    )(weights, span_values, acc, inverse, residual)


def close_kernel(
    w_ref, v_ref, part_ref, inv_ref, hid_ref, sum_ref, mine, others, send_sem, recv_sem
):
    devices, me = lax.axis_size("tp"), lax.axis_index("tp")
    ahead = [{"tp": lax.rem(me + k, devices)} for k in range(1, devices)]
    barrier = pltpu.get_barrier_semaphore()
    for peer in ahead:
        pl.semaphore_signal(barrier, inc=1, device_id=peer, device_id_type=MESH)

    key_heads, rows, _ = w_ref.shape
    count = part_ref.shape[0]
    head = v_ref.shape[1]
    squares = jnp.zeros((count, head), jnp.float32)
    for g in range(key_heads):
        mixed = jnp.dot(w_ref[g], v_ref[...], preferred_element_type=jnp.float32) * inv_ref[g]
        for h in range(rows // count):
            at = (g * (rows // count) + h) * head
            hidden = part_ref[:, at : at + head] + mixed[h * count : (h + 1) * count]
            hid_ref[:, at : at + head] = hidden
            squares = squares + hidden * hidden
    sums = jnp.sum(squares, axis=1, keepdims=True)
    lane = lax.broadcasted_iota(jnp.int32, mine.shape, 1)
    tile = jnp.zeros(mine.shape, jnp.float32)
    for k in range(count // mine.shape[0]):
        tile = jnp.where(lane == k, sums[k * mine.shape[0] : (k + 1) * mine.shape[0]], tile)
    mine[...] = tile
    pl.semaphore_wait(barrier, devices - 1)
    copies = [
        pltpu.make_async_remote_copy(
            src_ref=mine,
            dst_ref=others.at[k],
            send_sem=send_sem.at[k],
            recv_sem=recv_sem.at[k],
            device_id=peer,
            device_id_type=MESH,
        )
        for k, peer in enumerate(ahead)
    ]
    for copy in copies:
        copy.start()
    for k, copy in enumerate(copies):
        copy.wait_recv()
        tile = tile + others[k]
    sum_ref[...] = tile
    for copy in copies:
        copy.wait_send()


def close(weights, values, part, inverse):
    count, width = part.shape
    key_heads, rows, span = weights.shape
    head = values.shape[1]
    peers = lax.axis_size("tp") - 1
    vmem = pl.BlockSpec(memory_space=pltpu.VMEM)
    return pl.pallas_call(
        close_kernel,
        in_specs=[vmem] * 4,
        out_specs=[vmem] * 2,
        out_shape=[
            jax.ShapeDtypeStruct((count, width), jnp.float32),
            jax.ShapeDtypeStruct((8, head), jnp.float32),
        ],
        scratch_shapes=[
            pltpu.VMEM((8, head), jnp.float32),
            pltpu.VMEM((peers, 8, head), jnp.float32),
            pltpu.SemaphoreType.DMA((peers,)),
            pltpu.SemaphoreType.DMA((peers,)),
        ],
        compiler_params=pltpu.CompilerParams(
            collective_id=0, has_side_effects=True, vmem_limit_bytes=40 * 2**20
        ),
        cost_estimate=pl.CostEstimate(
            flops=4 * key_heads * rows * span * head, bytes_accessed=4 * 2**20, transcendentals=0
        ),
        name="close",
    )(weights, values, part, inverse)


def write_kernel(
    width, hid_ref, sum_ref, gain_ref, s_ref, t_ref, hv_in, out_ref, hv_ref, buffer, sems
):
    del hv_in
    ends = hv_ref.shape[0]
    moves = []
    for v_ref in (t_ref, s_ref):
        ends -= v_ref.shape[0]
        moves.append(
            pltpu.make_async_copy(v_ref, hv_ref.at[pl.ds(ends, v_ref.shape[0])], sems.at[len(moves)])
        )
        moves[-1].start()
    scale = lax.rsqrt(sum_ref[...] / width + epsilon)
    tall = scale.shape[0]
    step = 2 * tall
    for start in range(0, hid_ref.shape[0], step):
        rows = slice(start, start + step)
        first = start // tall
        each = jnp.concatenate([scale[:, first + k : first + k + 1] for k in range(2)], axis=0)
        buffer[rows, :] = (hid_ref[rows, :] * each * gain_ref[...]).astype(jnp.bfloat16)
        moves.append(
            pltpu.make_async_copy(
                buffer.at[pl.ds(start, step)], out_ref.at[pl.ds(start, step)], sems.at[len(moves)]
            )
        )
        moves[-1].start()
    for move in moves:
        move.wait()


def write(hidden, sums, gain, values, last_values, handed):
    count, columns = hidden.shape
    vmem = pl.BlockSpec(memory_space=pltpu.VMEM)
    anywhere = pl.BlockSpec(memory_space=pl.ANY)
    return pl.pallas_call(
        functools.partial(write_kernel, columns * lax.axis_size("tp")),
        in_specs=[vmem] * 5 + [anywhere],
        out_specs=[anywhere] * 2,
        out_shape=[
            jax.ShapeDtypeStruct((count, columns), jnp.bfloat16),
            jax.ShapeDtypeStruct(handed.shape, jnp.bfloat16),
        ],
        scratch_shapes=[
            pltpu.VMEM((count, columns), jnp.bfloat16),
            pltpu.SemaphoreType.DMA((2 + count // 16,)),
        ],
        input_output_aliases={5: 1},
        compiler_params=pltpu.CompilerParams(vmem_limit_bytes=40 * 2**20),
        cost_estimate=pl.CostEstimate(
            flops=8 * count * columns, bytes_accessed=2 * 2**20, transcendentals=0
        ),
        name="write",
    )(hidden, sums, gain, values, last_values, handed)


def normed(hidden, partial, gain):
    width = hidden.shape[1] * lax.axis_size("tp")
    squares = lax.psum(jnp.sum(partial, axis=1), "tp")
    scaled = hidden * lax.rsqrt(squares[:, None] / width + epsilon) * gain.astype(jnp.float32)
    return scaled.astype(jnp.bfloat16)


def local(
    prompt_keys,
    prompt_values,
    span_queries,
    span_keys,
    span_values,
    prefill_residual,
    decode_queries,
    decode_keys,
    decode_values,
    decode_residual,
    cursor,
    norm_gain,
):
    halfway = lax.axis_size("pair") // 2
    span, heads, head = span_queries.shape[1:]
    past, key_heads = prompt_keys.shape[1:3]
    steps, count = decode_keys.shape[1:3]
    group = heads // key_heads
    flat = lambda a: a.reshape(-1, head)
    far = []
    early, most = span // 2, past - past // 3
    pieces = (
        prompt_keys,
        span_keys,
        prompt_values[:, :most],
        prompt_values[:, most:],
        span_values[:, :early],
        span_values[:, early:],
    )
    for piece in pieces:
        far.append(from_behind(flat(piece), "pair", halfway))
    far_pk, far_sk, far_pv, far_qv, far_sv, far_tv = far

    keys = jnp.concatenate([prompt_keys[0], span_keys[0]], axis=0).transpose(1, 0, 2)
    values = jnp.concatenate([prompt_values[0], span_values[0]], axis=0).transpose(1, 0, 2)
    queries = span_queries[0].transpose(1, 0, 2)
    prefill_hidden, prefill_partial = prefill(queries, keys, values, prefill_residual[0])
    prefill_out = normed(prefill_hidden, prefill_partial, norm_gain)

    dq = decode_queries[0].reshape(steps * count, heads, head).transpose(1, 0, 2)
    dq = dq.reshape(key_heads, group * steps * count, head)
    dk = decode_keys[0].transpose(2, 0, 1, 3)
    dv = decode_values[0].transpose(2, 0, 1, 3)
    block = steps * count * (2 if group % 2 == 0 else 1)
    reach = jnp.tile(cursor[0], block // count)[:, None]
    prefill_out, dq, dk, dv, reach = lax.optimization_barrier((prefill_out, dq, dk, dv, reach))
    weights, ending, inverse, own, handed_keys = weigh(
        dq, far_pk, far_sk, dk, dv, reach, far_tv.shape[0]
    )
    acc, handed = mix(weights, far_pv, own, (past + span) * key_heads)
    acc, handed = mix_more(weights, far_qv, acc, handed, most * key_heads)
    residual = decode_residual[0].reshape(steps * count, heads * head)
    part = gather(weights, far_sv, acc, inverse, residual)
    decode_hidden, sums = close(ending, far_tv, part, inverse)
    gain = norm_gain.astype(jnp.float32)[None, :]
    decode_out, handed_values = write(decode_hidden, sums, gain, far_sv, far_tv, handed)
    shape = (1, past + span, key_heads, head)
    return (
        prefill_out[None],
        handed_keys.reshape(shape),
        handed_values.reshape(shape),
        decode_out.reshape(decode_residual.shape),
    )


def solution(mesh):
    row = ("groups", "pair")
    placed = (
        P(row, None, "tp", None),
        P(row, None, "tp", None),
        P(row, None, "tp", None),
        P(row, None, "tp", None),
        P(row, None, "tp", None),
        P(row, None, "tp"),
        P(row, None, None, "tp", None),
        P(row, None, None, "tp", None),
        P(row, None, None, "tp", None),
        P(row, None, None, "tp"),
        P(row, None),
        P("tp"),
    )
    return jax.shard_map(
        local,
        mesh=mesh,
        in_specs=placed,
        out_specs=(
            P(row, None, "tp"),
            P(row, None, "tp", None),
            P(row, None, "tp", None),
            P(row, None, None, "tp"),
        ),
        check_vma=False,
    )
```

```python
import functools

import jax
import jax.numpy as jnp
from jax import lax
from jax.experimental import pallas as pl
from jax.experimental.pallas import tpu as pltpu
from jax.sharding import PartitionSpec as P


epsilon = 1e-05
FIRST = ("half_pk", "half_sk", "half_pv", "half_sv")
SECOND = ("full_pk", "full_sk", "full_pv", "full_sv", "full_tv")
CROSS = FIRST[2:] + SECOND[2:]
NT = (((1,), (1,)), ((), ()))
MESH = pl.DeviceIdType.MESH


def routes(count):
    half, quarter = count // 2, count // 4
    if count % 4:
        first = [(place, (place + half) % count) for place in range(count)]
        return first, [(place, place) for place in range(count)]
    first, second = [], []
    for place in range(count):
        outer = place < quarter or place >= count - quarter
        step = quarter if outer else half
        first.append((place, place + step if place < half else place - step))
        second.append((place, place if outer else place + quarter if place < half else place - quarter))
    return first, second


def crossed(value, pairs):
    wide = lax.axis_size("tp")
    other = [t if wide % 2 else t + 1 - 2 * (t % 2) for t in range(wide)]
    both = [(a * wide + t, b * wide + other[t]) for a, b in pairs for t in range(wide)]
    return lax.ppermute(value, ("pair", "tp"), both)


def prefill_kernel(block, past, scale, q_ref, k_ref, v_ref, res_ref, hid_ref, sq_ref):
    span, _ = q_ref.shape[1:]

    @pl.when(pl.program_id(0) == 0)
    def _():
        sq_ref[...] = jnp.zeros_like(sq_ref)

    for start in range(0, span, block):
        rows = slice(start, start + block)
        reach = past + start + block
        scores = lax.dot_general(
            q_ref[0, rows, :], k_ref[0, :reach, :], NT, preferred_element_type=jnp.float32
        )
        row = lax.broadcasted_iota(jnp.int32, (block, block), 0)
        col = lax.broadcasted_iota(jnp.int32, (block, block), 1)
        last = jnp.where(col <= row, scores[:, reach - block :], -jnp.inf)
        scores = jnp.concatenate([scores[:, : reach - block], last], axis=1)
        peak = jnp.max(scores, axis=1, keepdims=True)
        weights = jnp.exp((scores - peak) * scale)
        total = jnp.sum(weights, axis=1, keepdims=True)
        mixed = jnp.dot(
            weights.astype(jnp.bfloat16), v_ref[0, :reach, :], preferred_element_type=jnp.float32
        )
        hidden = mixed / total + res_ref[rows, :].astype(jnp.float32)
        hid_ref[rows, :] = hidden
        sq_ref[rows, :] += hidden * hidden


def prefill(queries, keys, values, residual, first, last):
    heads, span, head = queries.shape
    key_heads, positions, _ = keys.shape
    group = heads // key_heads
    block = min(256, span)
    return pl.pallas_call(
        functools.partial(prefill_kernel, block, positions - span, head ** (-0.5)),
        grid=(last - first,),
        in_specs=[
            pl.BlockSpec((1, span, head), lambda h: (first + h, 0, 0)),
            pl.BlockSpec((1, positions, head), lambda h: ((first + h) // group, 0, 0)),
            pl.BlockSpec((1, positions, head), lambda h: ((first + h) // group, 0, 0)),
            pl.BlockSpec((span, head), lambda h: (0, first + h)),
        ],
        out_specs=[
            pl.BlockSpec((span, head), lambda h: (0, h)),
            pl.BlockSpec((span, head), lambda h: (0, 0)),
        ],
        out_shape=[
            jax.ShapeDtypeStruct((span, (last - first) * head), jnp.float32),
            jax.ShapeDtypeStruct((span, head), jnp.float32),
        ],
        compiler_params=pltpu.CompilerParams(vmem_limit_bytes=40 * 2**20),
        cost_estimate=pl.CostEstimate(
            flops=8 * (last - first) * span * positions * head,
            bytes_accessed=8 * 2**20,
            transcendentals=(last - first) * span * positions,
        ),
        name="prefill",
    )(queries, keys, values, residual)


def weigh_kernel(
    scale, key_heads, steps, q_ref, pk_ref, sk_ref, dk_ref, dv_ref, cur_ref,
    w_ref, last_ref, inv_ref, own_ref, hk_ref,
):
    g = pl.program_id(0)
    first = jnp.logical_and(g == 0, pl.program_id(1) == 0)
    past = pk_ref.shape[0]

    @pl.when(first)
    def _():
        hk_ref[:past, :] = pk_ref[...]
        hk_ref[past:, :] = sk_ref[...]

    q = q_ref[0]
    rows = q.shape[0]
    scores = jnp.concatenate(
        [
            lax.dot_general(q, pk_ref[...], NT, preferred_element_type=jnp.float32),
            lax.dot_general(q, sk_ref[...], NT, preferred_element_type=jnp.float32),
        ],
        axis=1,
    )
    col = lax.broadcasted_iota(jnp.int32, scores.shape, 1)
    seen = jnp.logical_and(col % key_heads == g, col < cur_ref[...] * key_heads)
    scores = jnp.where(seen, scores, -jnp.inf)
    peak = jnp.max(scores, axis=1, keepdims=True)
    count = dk_ref.shape[2]
    copies = rows // count
    step = lax.broadcasted_iota(jnp.int32, (rows, 1), 0) // count % steps
    wide = q.astype(jnp.float32)
    own_scores = []
    for u in range(steps):
        key = jnp.concatenate([dk_ref[0, u].astype(jnp.float32)] * copies, axis=0)
        own = jnp.sum(wide * key, axis=1, keepdims=True)
        own = jnp.where(step >= u, own, -jnp.inf)
        own_scores.append(own)
        peak = jnp.maximum(peak, own)
    weights = jnp.exp((scores - peak) * scale)
    total = jnp.sum(weights, axis=1, keepdims=True)
    rounded = weights.astype(jnp.bfloat16)
    w_ref[0] = rounded[:, : w_ref.shape[2]]
    last_ref[0] = rounded[:, w_ref.shape[2] :]
    mixed = jnp.zeros(wide.shape, jnp.float32)
    for u in range(steps):
        value = jnp.concatenate([dv_ref[0, u].astype(jnp.float32)] * copies, axis=0)
        weight = jnp.exp((own_scores[u] - peak) * scale)
        total = total + weight
        mixed = mixed + weight.astype(jnp.bfloat16).astype(jnp.float32) * value
    inv_ref[0] = jnp.broadcast_to(1.0 / total, wide.shape)
    own_ref[0] = mixed


def weigh(queries, prompt_keys, span_keys, own_keys, own_values, reach, ending):
    key_heads, rows, head = queries.shape
    _, steps, count, _ = own_keys.shape
    past, span = prompt_keys.shape[0], span_keys.shape[0]
    block = reach.shape[0]
    return pl.pallas_call(
        functools.partial(weigh_kernel, head ** (-0.5), key_heads, steps),
        grid=(key_heads, rows // block),
        in_specs=[
            pl.BlockSpec((1, block, head), lambda g, i: (g, i, 0)),
            pl.BlockSpec((past, head), lambda g, i: (0, 0)),
            pl.BlockSpec((span, head), lambda g, i: (0, 0)),
            pl.BlockSpec((1, steps, count, head), lambda g, i: (g, 0, 0, 0)),
            pl.BlockSpec((1, steps, count, head), lambda g, i: (g, 0, 0, 0)),
            pl.BlockSpec((block, 1), lambda g, i: (0, 0)),
        ],
        out_specs=[
            pl.BlockSpec((1, block, past + span - ending), lambda g, i: (g, i, 0)),
            pl.BlockSpec((1, block, ending), lambda g, i: (g, i, 0)),
            pl.BlockSpec((1, block, head), lambda g, i: (g, i, 0)),
            pl.BlockSpec((1, block, head), lambda g, i: (g, i, 0)),
            pl.BlockSpec((past + span, head), lambda g, i: (0, 0)),
        ],
        out_shape=[
            jax.ShapeDtypeStruct((key_heads, rows, past + span - ending), jnp.bfloat16),
            jax.ShapeDtypeStruct((key_heads, rows, ending), jnp.bfloat16),
            jax.ShapeDtypeStruct((key_heads, rows, head), jnp.float32),
            jax.ShapeDtypeStruct((key_heads, rows, head), jnp.float32),
            jax.ShapeDtypeStruct((past + span, head), jnp.bfloat16),
        ],
        compiler_params=pltpu.CompilerParams(vmem_limit_bytes=40 * 2**20),
        cost_estimate=pl.CostEstimate(
            flops=4 * key_heads * rows * (past + span) * head,
            bytes_accessed=16 * 2**20,
            transcendentals=key_heads * rows * (past + span),
        ),
        name="weigh",
    )(queries, prompt_keys, span_keys, own_keys, own_values, reach)


def mix_kernel(w_ref, v_ref, own_ref, acc_ref, hv_ref):
    @pl.when(pl.program_id(0) == 0)
    def _():
        hv_ref[...] = v_ref[...]

    acc_ref[0] = own_ref[0] + jnp.dot(w_ref[0], v_ref[...], preferred_element_type=jnp.float32)


def mix(weights, prompt_values, own, both):
    key_heads, rows, _ = weights.shape
    past, head = prompt_values.shape
    return pl.pallas_call(
        mix_kernel,
        grid=(key_heads,),
        in_specs=[
            pl.BlockSpec((1, rows, past), lambda g: (g, 0, 0)),
            pl.BlockSpec((past, head), lambda g: (0, 0)),
            pl.BlockSpec((1, rows, head), lambda g: (g, 0, 0)),
        ],
        out_specs=[
            pl.BlockSpec((1, rows, head), lambda g: (g, 0, 0)),
            pl.BlockSpec((past, head), lambda g: (0, 0)),
        ],
        out_shape=[
            jax.ShapeDtypeStruct((key_heads, rows, head), jnp.float32),
            jax.ShapeDtypeStruct((both, head), jnp.bfloat16),
        ],
        compiler_params=pltpu.CompilerParams(vmem_limit_bytes=40 * 2**20),
        cost_estimate=pl.CostEstimate(
            flops=4 * key_heads * rows * past * head, bytes_accessed=8 * 2**20, transcendentals=0
        ),
        name="mix",
    )(weights, prompt_values, own)


def gather_kernel(w_ref, v_ref, acc_ref, inv_ref, res_ref, part_ref):
    mixed = acc_ref[0] + jnp.dot(w_ref[0], v_ref[...], preferred_element_type=jnp.float32)
    mixed = mixed * inv_ref[0]
    count = res_ref.shape[0]
    head = mixed.shape[1]
    for h in range(mixed.shape[0] // count):
        columns = slice(h * head, (h + 1) * head)
        part_ref[:, columns] = mixed[h * count : (h + 1) * count] + res_ref[:, columns].astype(jnp.float32)


def gather(weights, span_values, acc, inverse, residual):
    key_heads, rows, columns = weights.shape
    span, head = span_values.shape
    count, width = residual.shape
    at = columns // span - 1
    return pl.pallas_call(
        gather_kernel,
        grid=(key_heads,),
        in_specs=[
            pl.BlockSpec((1, rows, span), lambda g: (g, 0, at)),
            pl.BlockSpec((span, head), lambda g: (0, 0)),
            pl.BlockSpec((1, rows, head), lambda g: (g, 0, 0)),
            pl.BlockSpec((1, rows, head), lambda g: (g, 0, 0)),
            pl.BlockSpec((count, width // key_heads), lambda g: (0, g)),
        ],
        out_specs=pl.BlockSpec((count, width // key_heads), lambda g: (0, g)),
        out_shape=jax.ShapeDtypeStruct((count, width), jnp.float32),
        compiler_params=pltpu.CompilerParams(vmem_limit_bytes=40 * 2**20),
        cost_estimate=pl.CostEstimate(
            flops=4 * key_heads * rows * span * head, bytes_accessed=6 * 2**20, transcendentals=0
        ),
        name="gather",
    )(weights, span_values, acc, inverse, residual)


def close_kernel(
    w_ref, v_ref, part_ref, inv_ref, hid_ref, sum_ref, mine, others, send_sem, recv_sem
):
    devices, me = lax.axis_size("tp"), lax.axis_index("tp")
    ahead = [{"tp": lax.rem(me + k, devices)} for k in range(1, devices)]
    barrier = pltpu.get_barrier_semaphore()
    for peer in ahead:
        pl.semaphore_signal(barrier, inc=1, device_id=peer, device_id_type=MESH)

    key_heads, rows, _ = w_ref.shape
    count = part_ref.shape[0]
    head = v_ref.shape[1]
    squares = jnp.zeros((count, head), jnp.float32)
    for g in range(key_heads):
        mixed = jnp.dot(w_ref[g], v_ref[...], preferred_element_type=jnp.float32) * inv_ref[g]
        for h in range(rows // count):
            at = (g * (rows // count) + h) * head
            hidden = part_ref[:, at : at + head] + mixed[h * count : (h + 1) * count]
            hid_ref[:, at : at + head] = hidden
            squares = squares + hidden * hidden
    sums = jnp.sum(squares, axis=1, keepdims=True)
    lane = lax.broadcasted_iota(jnp.int32, mine.shape, 1)
    tile = jnp.zeros(mine.shape, jnp.float32)
    for k in range(count // mine.shape[0]):
        tile = jnp.where(lane == k, sums[k * mine.shape[0] : (k + 1) * mine.shape[0]], tile)
    mine[...] = tile
    pl.semaphore_wait(barrier, devices - 1)
    copies = [
        pltpu.make_async_remote_copy(
            src_ref=mine,
            dst_ref=others.at[k],
            send_sem=send_sem.at[k],
            recv_sem=recv_sem.at[k],
            device_id=peer,
            device_id_type=MESH,
        )
        for k, peer in enumerate(ahead)
    ]
    for copy in copies:
        copy.start()
    for k, copy in enumerate(copies):
        copy.wait_recv()
        tile = tile + others[k]
    sum_ref[...] = tile
    for copy in copies:
        copy.wait_send()


def close(weights, values, part, inverse):
    count, width = part.shape
    key_heads, rows, span = weights.shape
    head = values.shape[1]
    peers = lax.axis_size("tp") - 1
    vmem = pl.BlockSpec(memory_space=pltpu.VMEM)
    return pl.pallas_call(
        close_kernel,
        in_specs=[vmem] * 4,
        out_specs=[vmem] * 2,
        out_shape=[
            jax.ShapeDtypeStruct((count, width), jnp.float32),
            jax.ShapeDtypeStruct((8, head), jnp.float32),
        ],
        scratch_shapes=[
            pltpu.VMEM((8, head), jnp.float32),
            pltpu.VMEM((peers, 8, head), jnp.float32),
            pltpu.SemaphoreType.DMA((peers,)),
            pltpu.SemaphoreType.DMA((peers,)),
        ],
        compiler_params=pltpu.CompilerParams(
            collective_id=0, has_side_effects=True, vmem_limit_bytes=40 * 2**20
        ),
        cost_estimate=pl.CostEstimate(
            flops=4 * key_heads * rows * span * head, bytes_accessed=4 * 2**20, transcendentals=0
        ),
        name="close",
    )(weights, values, part, inverse)


def write_kernel(
    width, hid_ref, sum_ref, gain_ref, s_ref, t_ref, hv_in, out_ref, hv_ref, buffer, sems
):
    del hv_in
    ends = hv_ref.shape[0]
    moves = []
    for v_ref in (t_ref, s_ref):
        ends -= v_ref.shape[0]
        moves.append(
            pltpu.make_async_copy(v_ref, hv_ref.at[pl.ds(ends, v_ref.shape[0])], sems.at[len(moves)])
        )
        moves[-1].start()
    scale = lax.rsqrt(sum_ref[...] / width + epsilon)
    tall = scale.shape[0]
    step = 2 * tall
    for start in range(0, hid_ref.shape[0], step):
        rows = slice(start, start + step)
        first = start // tall
        each = jnp.concatenate([scale[:, first + k : first + k + 1] for k in range(2)], axis=0)
        buffer[rows, :] = (hid_ref[rows, :] * each * gain_ref[...]).astype(jnp.bfloat16)
        moves.append(
            pltpu.make_async_copy(
                buffer.at[pl.ds(start, step)], out_ref.at[pl.ds(start, step)], sems.at[len(moves)]
            )
        )
        moves[-1].start()
    for move in moves:
        move.wait()


def write(hidden, sums, gain, values, last_values, handed):
    count, columns = hidden.shape
    vmem = pl.BlockSpec(memory_space=pltpu.VMEM)
    anywhere = pl.BlockSpec(memory_space=pl.ANY)
    return pl.pallas_call(
        functools.partial(write_kernel, columns * lax.axis_size("tp")),
        in_specs=[vmem] * 5 + [anywhere],
        out_specs=[anywhere] * 2,
        out_shape=[
            jax.ShapeDtypeStruct((count, columns), jnp.bfloat16),
            jax.ShapeDtypeStruct(handed.shape, jnp.bfloat16),
        ],
        scratch_shapes=[
            pltpu.VMEM((count, columns), jnp.bfloat16),
            pltpu.SemaphoreType.DMA((2 + count // 16,)),
        ],
        input_output_aliases={5: 1},
        compiler_params=pltpu.CompilerParams(vmem_limit_bytes=40 * 2**20),
        cost_estimate=pl.CostEstimate(
            flops=8 * count * columns, bytes_accessed=2 * 2**20, transcendentals=0
        ),
        name="write",
    )(hidden, sums, gain, values, last_values, handed)


def normed(hidden, partial, gain):
    columns = sum(part.shape[1] for part in hidden)
    width = columns * lax.axis_size("tp")
    squares = lax.psum(jnp.sum(sum(partial), axis=1), "tp")
    inverse = lax.rsqrt(squares[:, None] / width + epsilon)
    out, at = [], 0
    for part in hidden:
        here = gain[at : at + part.shape[1]].astype(jnp.float32)
        out.append((part * inverse * here).astype(jnp.bfloat16))
        at += part.shape[1]
    return jnp.concatenate(out, axis=1)


def local(
    prompt_keys,
    prompt_values,
    span_queries,
    span_keys,
    span_values,
    prefill_residual,
    decode_queries,
    decode_keys,
    decode_values,
    decode_residual,
    cursor,
    norm_gain,
):
    span, heads, head = span_queries.shape[1:]
    past, key_heads = prompt_keys.shape[1:3]
    steps, count = decode_keys.shape[1:3]
    group = heads // key_heads
    flat = lambda a: a.reshape(-1, head)
    first, second = routes(lax.axis_size("pair"))
    half_way, far = [], []
    for name, piece in zip(FIRST, (prompt_keys, span_keys, prompt_values, span_values)):
        if name in CROSS:
            half_way.append(crossed(flat(piece), first))
        else:
            half_way.append(lax.ppermute(flat(piece), "pair", first))
    keys = jnp.concatenate([prompt_keys[0], span_keys[0]], axis=0).transpose(1, 0, 2)
    values = jnp.concatenate([prompt_values[0], span_values[0]], axis=0).transpose(1, 0, 2)
    queries = span_queries[0].transpose(1, 0, 2)
    hidden, partial = [], []
    cuts = (0, heads // 2, heads)
    for start, stop in zip(cuts, cuts[1:]):
        done = prefill(queries, keys, values, prefill_residual[0], start, stop)
        hidden.append(done[0])
        partial.append(done[1])
    partial[-1], later = lax.optimization_barrier((partial[-1], half_way[-1]))
    early = span // 2 * key_heads
    far = []
    for name, piece in zip(SECOND, half_way[:-1] + [later[:early], later[early:]]):
        if name in CROSS:
            far.append(crossed(piece, second))
        else:
            far.append(lax.ppermute(piece, "pair", second))
    far_pk, far_sk, far_pv, far_sv, far_tv = far
    prefill_out = normed(hidden, partial, norm_gain)

    dq = decode_queries[0].reshape(steps * count, heads, head).transpose(1, 0, 2)
    dq = dq.reshape(key_heads, group * steps * count, head)
    dk = decode_keys[0].transpose(2, 0, 1, 3)
    dv = decode_values[0].transpose(2, 0, 1, 3)
    block = steps * count * (2 if group % 2 == 0 else 1)
    reach = jnp.tile(cursor[0], block // count)[:, None]
    prefill_out, dq, dk, dv, reach = lax.optimization_barrier((prefill_out, dq, dk, dv, reach))
    weights, ending, inverse, own, handed_keys = weigh(
        dq, far_pk, far_sk, dk, dv, reach, far_tv.shape[0]
    )
    acc, handed = mix(weights, far_pv, own, (past + span) * key_heads)
    residual = decode_residual[0].reshape(steps * count, heads * head)
    part = gather(weights, far_sv, acc, inverse, residual)
    decode_hidden, sums = close(ending, far_tv, part, inverse)
    gain = norm_gain.astype(jnp.float32)[None, :]
    decode_out, handed_values = write(decode_hidden, sums, gain, far_sv, far_tv, handed)
    shape = (1, past + span, key_heads, head)
    return (
        prefill_out[None],
        handed_keys.reshape(shape),
        handed_values.reshape(shape),
        decode_out.reshape(decode_residual.shape),
    )


def solution(mesh):
    row = ("groups", "pair")
    placed = (
        P(row, None, "tp", None),
        P(row, None, "tp", None),
        P(row, None, "tp", None),
        P(row, None, "tp", None),
        P(row, None, "tp", None),
        P(row, None, "tp"),
        P(row, None, None, "tp", None),
        P(row, None, None, "tp", None),
        P(row, None, None, "tp", None),
        P(row, None, None, "tp"),
        P(row, None),
        P("tp"),
    )
    return jax.shard_map(
        local,
        mesh=mesh,
        in_specs=placed,
        out_specs=(
            P(row, None, "tp"),
            P(row, None, "tp", None),
            P(row, None, "tp", None),
            P(row, None, None, "tp"),
        ),
        check_vma=False,
    )
```

```python
import functools

import jax
import jax.numpy as jnp
from jax import lax
from jax.experimental import pallas as pl
from jax.experimental.pallas import tpu as pltpu
from jax.sharding import PartitionSpec as P


epsilon = 1e-05
FIRST = ("half_pk", "half_sk", "half_pv", "half_sv")
SECOND = ("full_pk", "full_sk", "full_pv", "full_sv")
CROSS = FIRST[2:] + SECOND[2:]
NT = (((1,), (1,)), ((), ()))
MESH = pl.DeviceIdType.MESH


def routes(count):
    half, quarter = count // 2, count // 4
    if count % 4:
        first = [(place, (place + half) % count) for place in range(count)]
        return first, [(place, place) for place in range(count)]
    first, second = [], []
    for place in range(count):
        outer = place < quarter or place >= count - quarter
        step = quarter if outer else half
        first.append((place, place + step if place < half else place - step))
        second.append((place, place if outer else place + quarter if place < half else place - quarter))
    return first, second


def crossed(value, pairs):
    wide = lax.axis_size("tp")
    other = [t if wide % 2 else t + 1 - 2 * (t % 2) for t in range(wide)]
    both = [(a * wide + t, b * wide + other[t]) for a, b in pairs for t in range(wide)]
    return lax.ppermute(value, ("pair", "tp"), both)


def prefill_kernel(block, past, scale, q_ref, k_ref, v_ref, res_ref, hid_ref, sq_ref):
    span, _ = q_ref.shape[1:]

    @pl.when(pl.program_id(0) == 0)
    def _():
        sq_ref[...] = jnp.zeros_like(sq_ref)

    for start in range(0, span, block):
        rows = slice(start, start + block)
        reach = past + start + block
        scores = lax.dot_general(
            q_ref[0, rows, :], k_ref[0, :reach, :], NT, preferred_element_type=jnp.float32
        )
        row = lax.broadcasted_iota(jnp.int32, (block, block), 0)
        col = lax.broadcasted_iota(jnp.int32, (block, block), 1)
        last = jnp.where(col <= row, scores[:, reach - block :], -jnp.inf)
        scores = jnp.concatenate([scores[:, : reach - block], last], axis=1)
        peak = jnp.max(scores, axis=1, keepdims=True)
        weights = jnp.exp((scores - peak) * scale)
        total = jnp.sum(weights, axis=1, keepdims=True)
        mixed = jnp.dot(
            weights.astype(jnp.bfloat16), v_ref[0, :reach, :], preferred_element_type=jnp.float32
        )
        hidden = mixed / total + res_ref[rows, :].astype(jnp.float32)
        hid_ref[rows, :] = hidden
        sq_ref[rows, :] += hidden * hidden


def prefill(queries, keys, values, residual, first, last):
    heads, span, head = queries.shape
    key_heads, positions, _ = keys.shape
    group = heads // key_heads
    block = min(256, span)
    return pl.pallas_call(
        functools.partial(prefill_kernel, block, positions - span, head ** (-0.5)),
        grid=(last - first,),
        in_specs=[
            pl.BlockSpec((1, span, head), lambda h: (first + h, 0, 0)),
            pl.BlockSpec((1, positions, head), lambda h: ((first + h) // group, 0, 0)),
            pl.BlockSpec((1, positions, head), lambda h: ((first + h) // group, 0, 0)),
            pl.BlockSpec((span, head), lambda h: (0, first + h)),
        ],
        out_specs=[
            pl.BlockSpec((span, head), lambda h: (0, h)),
            pl.BlockSpec((span, head), lambda h: (0, 0)),
        ],
        out_shape=[
            jax.ShapeDtypeStruct((span, (last - first) * head), jnp.float32),
            jax.ShapeDtypeStruct((span, head), jnp.float32),
        ],
        compiler_params=pltpu.CompilerParams(vmem_limit_bytes=40 * 2**20),
        cost_estimate=pl.CostEstimate(
            flops=8 * (last - first) * span * positions * head,
            bytes_accessed=8 * 2**20,
            transcendentals=(last - first) * span * positions,
        ),
        name="prefill",
    )(queries, keys, values, residual)


def weigh_kernel(
    scale, key_heads, steps, q_ref, pk_ref, sk_ref, dk_ref, dv_ref, cur_ref,
    w_ref, last_ref, inv_ref, own_ref, hk_ref,
):
    g = pl.program_id(0)
    first = jnp.logical_and(g == 0, pl.program_id(1) == 0)
    past = pk_ref.shape[0]

    @pl.when(first)
    def _():
        hk_ref[:past, :] = pk_ref[...]
        hk_ref[past:, :] = sk_ref[...]

    q = q_ref[0]
    rows = q.shape[0]
    scores = jnp.concatenate(
        [
            lax.dot_general(q, pk_ref[...], NT, preferred_element_type=jnp.float32),
            lax.dot_general(q, sk_ref[...], NT, preferred_element_type=jnp.float32),
        ],
        axis=1,
    )
    col = lax.broadcasted_iota(jnp.int32, scores.shape, 1)
    seen = jnp.logical_and(col % key_heads == g, col < cur_ref[...] * key_heads)
    scores = jnp.where(seen, scores, -jnp.inf)
    peak = jnp.max(scores, axis=1, keepdims=True)
    count = dk_ref.shape[2]
    copies = rows // count
    step = lax.broadcasted_iota(jnp.int32, (rows, 1), 0) // count % steps
    wide = q.astype(jnp.float32)
    own_scores = []
    for u in range(steps):
        key = jnp.concatenate([dk_ref[0, u].astype(jnp.float32)] * copies, axis=0)
        own = jnp.sum(wide * key, axis=1, keepdims=True)
        own = jnp.where(step >= u, own, -jnp.inf)
        own_scores.append(own)
        peak = jnp.maximum(peak, own)
    weights = jnp.exp((scores - peak) * scale)
    total = jnp.sum(weights, axis=1, keepdims=True)
    rounded = weights.astype(jnp.bfloat16)
    w_ref[0] = rounded[:, : w_ref.shape[2]]
    last_ref[0] = rounded[:, w_ref.shape[2] :]
    mixed = jnp.zeros(wide.shape, jnp.float32)
    for u in range(steps):
        value = jnp.concatenate([dv_ref[0, u].astype(jnp.float32)] * copies, axis=0)
        weight = jnp.exp((own_scores[u] - peak) * scale)
        total = total + weight
        mixed = mixed + weight.astype(jnp.bfloat16).astype(jnp.float32) * value
    inv_ref[0] = jnp.broadcast_to(1.0 / total, wide.shape)
    own_ref[0] = mixed


def weigh(queries, prompt_keys, span_keys, own_keys, own_values, reach, ending):
    key_heads, rows, head = queries.shape
    _, steps, count, _ = own_keys.shape
    past, span = prompt_keys.shape[0], span_keys.shape[0]
    block = reach.shape[0]
    return pl.pallas_call(
        functools.partial(weigh_kernel, head ** (-0.5), key_heads, steps),
        grid=(key_heads, rows // block),
        in_specs=[
            pl.BlockSpec((1, block, head), lambda g, i: (g, i, 0)),
            pl.BlockSpec((past, head), lambda g, i: (0, 0)),
            pl.BlockSpec((span, head), lambda g, i: (0, 0)),
            pl.BlockSpec((1, steps, count, head), lambda g, i: (g, 0, 0, 0)),
            pl.BlockSpec((1, steps, count, head), lambda g, i: (g, 0, 0, 0)),
            pl.BlockSpec((block, 1), lambda g, i: (0, 0)),
        ],
        out_specs=[
            pl.BlockSpec((1, block, past + span - ending), lambda g, i: (g, i, 0)),
            pl.BlockSpec((1, block, ending), lambda g, i: (g, i, 0)),
            pl.BlockSpec((1, block, head), lambda g, i: (g, i, 0)),
            pl.BlockSpec((1, block, head), lambda g, i: (g, i, 0)),
            pl.BlockSpec((past + span, head), lambda g, i: (0, 0)),
        ],
        out_shape=[
            jax.ShapeDtypeStruct((key_heads, rows, past + span - ending), jnp.bfloat16),
            jax.ShapeDtypeStruct((key_heads, rows, ending), jnp.bfloat16),
            jax.ShapeDtypeStruct((key_heads, rows, head), jnp.float32),
            jax.ShapeDtypeStruct((key_heads, rows, head), jnp.float32),
            jax.ShapeDtypeStruct((past + span, head), jnp.bfloat16),
        ],
        compiler_params=pltpu.CompilerParams(vmem_limit_bytes=40 * 2**20),
        cost_estimate=pl.CostEstimate(
            flops=4 * key_heads * rows * (past + span) * head,
            bytes_accessed=16 * 2**20,
            transcendentals=key_heads * rows * (past + span),
        ),
        name="weigh",
    )(queries, prompt_keys, span_keys, own_keys, own_values, reach)


def mix_kernel(w_ref, v_ref, own_ref, inv_ref, res_ref, part_ref, hv_ref):
    @pl.when(pl.program_id(0) == 0)
    def _():
        hv_ref[...] = v_ref[...]

    mixed = own_ref[0] + jnp.dot(w_ref[0], v_ref[...], preferred_element_type=jnp.float32)
    mixed = mixed * inv_ref[0]
    count = res_ref.shape[0]
    head = mixed.shape[1]
    for h in range(mixed.shape[0] // count):
        columns = slice(h * head, (h + 1) * head)
        part_ref[:, columns] = mixed[h * count : (h + 1) * count] + res_ref[:, columns].astype(jnp.float32)


def mix(weights, prompt_values, own, inverse, residual, both):
    key_heads, rows, _ = weights.shape
    past, head = prompt_values.shape
    count, width = residual.shape
    return pl.pallas_call(
        mix_kernel,
        grid=(key_heads,),
        in_specs=[
            pl.BlockSpec((1, rows, past), lambda g: (g, 0, 0)),
            pl.BlockSpec((past, head), lambda g: (0, 0)),
            pl.BlockSpec((1, rows, head), lambda g: (g, 0, 0)),
            pl.BlockSpec((1, rows, head), lambda g: (g, 0, 0)),
            pl.BlockSpec((count, width // key_heads), lambda g: (0, g)),
        ],
        out_specs=[
            pl.BlockSpec((count, width // key_heads), lambda g: (0, g)),
            pl.BlockSpec((past, head), lambda g: (0, 0)),
        ],
        out_shape=[
            jax.ShapeDtypeStruct((count, width), jnp.float32),
            jax.ShapeDtypeStruct((both, head), jnp.bfloat16),
        ],
        compiler_params=pltpu.CompilerParams(vmem_limit_bytes=40 * 2**20),
        cost_estimate=pl.CostEstimate(
            flops=4 * key_heads * rows * past * head, bytes_accessed=8 * 2**20, transcendentals=0
        ),
        name="mix",
    )(weights, prompt_values, own, inverse, residual)


def close_kernel(
    w_ref, v_ref, part_ref, inv_ref, hid_ref, sum_ref, mine, others, send_sem, recv_sem
):
    devices, me = lax.axis_size("tp"), lax.axis_index("tp")
    ahead = [{"tp": lax.rem(me + k, devices)} for k in range(1, devices)]
    barrier = pltpu.get_barrier_semaphore()
    for peer in ahead:
        pl.semaphore_signal(barrier, inc=1, device_id=peer, device_id_type=MESH)

    key_heads, rows, _ = w_ref.shape
    count = part_ref.shape[0]
    head = v_ref.shape[1]
    squares = jnp.zeros((count, head), jnp.float32)
    for g in range(key_heads):
        mixed = jnp.dot(w_ref[g], v_ref[...], preferred_element_type=jnp.float32) * inv_ref[g]
        for h in range(rows // count):
            at = (g * (rows // count) + h) * head
            hidden = part_ref[:, at : at + head] + mixed[h * count : (h + 1) * count]
            hid_ref[:, at : at + head] = hidden
            squares = squares + hidden * hidden
    sums = jnp.sum(squares, axis=1, keepdims=True)
    lane = lax.broadcasted_iota(jnp.int32, mine.shape, 1)
    tile = jnp.zeros(mine.shape, jnp.float32)
    for k in range(count // mine.shape[0]):
        tile = jnp.where(lane == k, sums[k * mine.shape[0] : (k + 1) * mine.shape[0]], tile)
    mine[...] = tile
    pl.semaphore_wait(barrier, devices - 1)
    copies = [
        pltpu.make_async_remote_copy(
            src_ref=mine,
            dst_ref=others.at[k],
            send_sem=send_sem.at[k],
            recv_sem=recv_sem.at[k],
            device_id=peer,
            device_id_type=MESH,
        )
        for k, peer in enumerate(ahead)
    ]
    for copy in copies:
        copy.start()
    for k, copy in enumerate(copies):
        copy.wait_recv()
        tile = tile + others[k]
    sum_ref[...] = tile
    for copy in copies:
        copy.wait_send()


def close(weights, values, part, inverse):
    count, width = part.shape
    key_heads, rows, span = weights.shape
    head = values.shape[1]
    peers = lax.axis_size("tp") - 1
    vmem = pl.BlockSpec(memory_space=pltpu.VMEM)
    return pl.pallas_call(
        close_kernel,
        in_specs=[vmem] * 4,
        out_specs=[vmem] * 2,
        out_shape=[
            jax.ShapeDtypeStruct((count, width), jnp.float32),
            jax.ShapeDtypeStruct((8, head), jnp.float32),
        ],
        scratch_shapes=[
            pltpu.VMEM((8, head), jnp.float32),
            pltpu.VMEM((peers, 8, head), jnp.float32),
            pltpu.SemaphoreType.DMA((peers,)),
            pltpu.SemaphoreType.DMA((peers,)),
        ],
        compiler_params=pltpu.CompilerParams(
            collective_id=0, has_side_effects=True, vmem_limit_bytes=40 * 2**20
        ),
        cost_estimate=pl.CostEstimate(
            flops=4 * key_heads * rows * span * head, bytes_accessed=4 * 2**20, transcendentals=0
        ),
        name="close",
    )(weights, values, part, inverse)


def write_kernel(
    width, hid_ref, sum_ref, gain_ref, s_ref, hv_in, out_ref, hv_ref, buffer, sems
):
    del hv_in
    ends = hv_ref.shape[0]
    moves = []
    for v_ref in (s_ref,):
        ends -= v_ref.shape[0]
        moves.append(
            pltpu.make_async_copy(v_ref, hv_ref.at[pl.ds(ends, v_ref.shape[0])], sems.at[len(moves)])
        )
        moves[-1].start()
    scale = lax.rsqrt(sum_ref[...] / width + epsilon)
    tall = scale.shape[0]
    step = 2 * tall
    for start in range(0, hid_ref.shape[0], step):
        rows = slice(start, start + step)
        first = start // tall
        each = jnp.concatenate([scale[:, first + k : first + k + 1] for k in range(2)], axis=0)
        buffer[rows, :] = (hid_ref[rows, :] * each * gain_ref[...]).astype(jnp.bfloat16)
        moves.append(
            pltpu.make_async_copy(
                buffer.at[pl.ds(start, step)], out_ref.at[pl.ds(start, step)], sems.at[len(moves)]
            )
        )
        moves[-1].start()
    for move in moves:
        move.wait()


def write(hidden, sums, gain, values, handed):
    count, columns = hidden.shape
    vmem = pl.BlockSpec(memory_space=pltpu.VMEM)
    anywhere = pl.BlockSpec(memory_space=pl.ANY)
    return pl.pallas_call(
        functools.partial(write_kernel, columns * lax.axis_size("tp")),
        in_specs=[vmem] * 4 + [anywhere],
        out_specs=[anywhere] * 2,
        out_shape=[
            jax.ShapeDtypeStruct((count, columns), jnp.bfloat16),
            jax.ShapeDtypeStruct(handed.shape, jnp.bfloat16),
        ],
        scratch_shapes=[
            pltpu.VMEM((count, columns), jnp.bfloat16),
            pltpu.SemaphoreType.DMA((2 + count // 16,)),
        ],
        input_output_aliases={4: 1},
        compiler_params=pltpu.CompilerParams(vmem_limit_bytes=40 * 2**20),
        cost_estimate=pl.CostEstimate(
            flops=8 * count * columns, bytes_accessed=2 * 2**20, transcendentals=0
        ),
        name="write",
    )(hidden, sums, gain, values, handed)


def normed(hidden, partial, gain):
    columns = sum(part.shape[1] for part in hidden)
    width = columns * lax.axis_size("tp")
    squares = lax.psum(jnp.sum(sum(partial), axis=1), "tp")
    inverse = lax.rsqrt(squares[:, None] / width + epsilon)
    out, at = [], 0
    for part in hidden:
        here = gain[at : at + part.shape[1]].astype(jnp.float32)
        out.append((part * inverse * here).astype(jnp.bfloat16))
        at += part.shape[1]
    return jnp.concatenate(out, axis=1)


def local(
    prompt_keys,
    prompt_values,
    span_queries,
    span_keys,
    span_values,
    prefill_residual,
    decode_queries,
    decode_keys,
    decode_values,
    decode_residual,
    cursor,
    norm_gain,
):
    span, heads, head = span_queries.shape[1:]
    past, key_heads = prompt_keys.shape[1:3]
    steps, count = decode_keys.shape[1:3]
    group = heads // key_heads
    flat = lambda a: a.reshape(-1, head)
    first, second = routes(lax.axis_size("pair"))
    half_way, far = [], []
    for name, piece in zip(FIRST, (prompt_keys, span_keys, prompt_values, span_values)):
        if name in CROSS:
            half_way.append(crossed(flat(piece), first))
        else:
            half_way.append(lax.ppermute(flat(piece), "pair", first))
    keys = jnp.concatenate([prompt_keys[0], span_keys[0]], axis=0).transpose(1, 0, 2)
    values = jnp.concatenate([prompt_values[0], span_values[0]], axis=0).transpose(1, 0, 2)
    queries = span_queries[0].transpose(1, 0, 2)
    hidden, partial = [], []
    cuts = (0, heads // 2, heads)
    for start, stop in zip(cuts, cuts[1:]):
        done = prefill(queries, keys, values, prefill_residual[0], start, stop)
        hidden.append(done[0])
        partial.append(done[1])
    partial[-1], later = lax.optimization_barrier((partial[-1], half_way[-1]))
    far = []
    for name, piece in zip(SECOND, half_way[:-1] + [later]):
        if name in CROSS:
            far.append(crossed(piece, second))
        else:
            far.append(lax.ppermute(piece, "pair", second))
    far_pk, far_sk, far_pv, far_sv = far
    prefill_out = normed(hidden, partial, norm_gain)

    dq = decode_queries[0].reshape(steps * count, heads, head).transpose(1, 0, 2)
    dq = dq.reshape(key_heads, group * steps * count, head)
    dk = decode_keys[0].transpose(2, 0, 1, 3)
    dv = decode_values[0].transpose(2, 0, 1, 3)
    block = steps * count * (2 if group % 2 == 0 else 1)
    reach = jnp.tile(cursor[0], block // count)[:, None]
    prefill_out, dq, dk, dv, reach = lax.optimization_barrier((prefill_out, dq, dk, dv, reach))
    weights, ending, inverse, own, handed_keys = weigh(
        dq, far_pk, far_sk, dk, dv, reach, far_sv.shape[0]
    )
    residual = decode_residual[0].reshape(steps * count, heads * head)
    part, handed = mix(weights, far_pv, own, inverse, residual, (past + span) * key_heads)
    decode_hidden, sums = close(ending, far_sv, part, inverse)
    gain = norm_gain.astype(jnp.float32)[None, :]
    decode_out, handed_values = write(decode_hidden, sums, gain, far_sv, handed)
    shape = (1, past + span, key_heads, head)
    return (
        prefill_out[None],
        handed_keys.reshape(shape),
        handed_values.reshape(shape),
        decode_out.reshape(decode_residual.shape),
    )


def solution(mesh):
    row = ("groups", "pair")
    placed = (
        P(row, None, "tp", None),
        P(row, None, "tp", None),
        P(row, None, "tp", None),
        P(row, None, "tp", None),
        P(row, None, "tp", None),
        P(row, None, "tp"),
        P(row, None, None, "tp", None),
        P(row, None, None, "tp", None),
        P(row, None, None, "tp", None),
        P(row, None, None, "tp"),
        P(row, None),
        P("tp"),
    )
    return jax.shard_map(
        local,
        mesh=mesh,
        in_specs=placed,
        out_specs=(
            P(row, None, "tp"),
            P(row, None, "tp", None),
            P(row, None, "tp", None),
            P(row, None, None, "tp"),
        ),
        check_vma=False,
    )
```
